32 devices in a mesh: sub: 16 (over z, y, x), crs: 2 (over core).
Axes of the slice: x: 2, y: 2, z: 4, core: 2. Of those that a mesh axis runs over, the one named last changes fastest.
Arguments:
- multipliers: float32 [16, 128, 512], P(None, ('sub', 'crs')), may hold values from -6 to 6
- own_modes: float32 [6, 128, 512], P(None, ('sub', 'crs')), may hold values from -0.75 to 0.75
- neighbour_modes: float32 [6, 128, 512], P(None, ('sub', 'crs')), may hold values from -0.75 to 0.75
- face_index: int32 [128, 512], P(('sub', 'crs')), may hold values from 0 to 5, as said below
- neighbour_list: int32 [128, 6], replicated, may hold values from 0 to 127, as said below
- coarse_factor: float32 [768, 768], P('sub', 'crs'), may hold values from -0.21875 to 0.21875
Outputs:
- projected: float32 [16, 128, 512], P(None, ('sub', 'crs'))
The draws below stay inside these ranges and needn't reach their ends.
Inputs may be any that keep to these rules, and one draw needn't show every extreme that they name: `face_index`: the multipliers of each subdomain lie in 6 contiguous nonempty blocks, face 0 first and face 5 last. `neighbour_list`: subdomain s = (8 x + y) * 8 + z sits at (x, y, z) of a periodic grid of 2 x 8 x 8 subdomains; the 6 faces of each subdomain name its grid neighbours x plus 1, x minus 1, y plus or minus 1, z plus or minus 1 (periodic; along the first dimension both name the same subdomain), in an order that differs from subdomain to subdomain.
All inputs are finite; a program needn't handle non-finite values.
Results may differ from the reference program's by a relative error of at most 0.0001.
Values sent between devices are 32-bit elements; how exact they have to be, the bound alone decides.
A program may use at most 64 MiB of HBM per device.

```python
import jax
import jax.numpy as jnp
from jax import lax

MODES = 6
NFACE = 6
IW = 512
NRHS = 16
NSUB = 128
NC = 768
GY = 8
GX = 2
GZ = 8


def draw_face_index(key, part):
    block = IW // NFACE
    spread = block // 4
    jitter = jax.random.randint(key, (NSUB, NFACE - 1), -spread, spread + 1).astype(jnp.int32)
    starts = (lax.broadcasted_iota(jnp.int32, (NSUB, NFACE - 1), 1) + 1) * block + jitter
    places = lax.broadcasted_iota(jnp.int32, (NSUB, IW), 1)
    passed = (places[:, :, None] >= starts[:, None, :]).astype(jnp.int32)
    return jnp.sum(passed, axis=2).astype(jnp.int32)


def draw_neighbour_list(key, part):
    scores = jax.random.randint(jax.random.fold_in(key, 17), (NSUB, NFACE), 0, 1 << 20).astype(jnp.int32)
    scores = scores * 8 + lax.broadcasted_iota(jnp.int32, (NSUB, NFACE), 1)
    order = jnp.argsort(scores, axis=1, stable=True).astype(jnp.int32)
    cells = lax.iota(jnp.int32, NSUB)
    first = cells // (GY * GZ)
    second = cells // GZ % GY
    third = cells % GZ

    def place(a, b, c):
        return ((a * GY + b) * GZ + c).astype(jnp.int32)
    table = jnp.stack([place((first + 1) % GX, second, third), place((first + GX - 1) % GX, second, third), place(first, (second + 1) % GY, third), place(first, (second + GY - 1) % GY, third), place(first, second, (third + 1) % GZ), place(first, second, (third + GZ - 1) % GZ)], axis=1)
    return jnp.take_along_axis(table, order, axis=1).astype(jnp.int32)


def levels(stream_key, dims, cuts, low, top_value):
    gain = 1.0
    for dim, parts in cuts:
        draws = jax.random.uniform(jax.random.fold_in(jax.random.fold_in(stream_key, 6), dim), (parts,), jnp.float32, low / len(cuts), top_value / len(cuts))
        gain = gain * jnp.repeat(jnp.exp(draws), dims[dim] // parts).reshape((-1,) + (1,) * (len(dims) - 1 - dim))
    return gain


def normal_values(key, shape, scale, most, shards=(), kind=jnp.bfloat16):
    array = jax.random.normal(key, shape, jnp.float32) * scale
    if len(shards) > 0:
        array = levels(key, shape, shards, -0.22, 0.18) * array
    return jnp.clip(array, min=-most, max=most).astype(kind)


def setup_inputs(seed: int = 0) -> dict:
    seeds = jax.random.split(jax.random.key(seed), 7)
    return {
        "multipliers": normal_values(seeds[0], (NRHS, NSUB, IW), 1.0, 6.0, ((1, 32),), jnp.float32),
        "own_modes": normal_values(seeds[1], (MODES, NSUB, IW), (IW // 8) ** -0.5, 0.75, ((1, 32),), jnp.float32),
        "neighbour_modes": normal_values(seeds[2], (MODES, NSUB, IW), (IW // 8) ** -0.5, 0.75, ((1, 32),), jnp.float32),
        "face_index": draw_face_index(jax.random.fold_in(seeds[6], 71), 0),
        "neighbour_list": draw_neighbour_list(jax.random.fold_in(seeds[6], 71), 0),
        "coarse_factor": normal_values(seeds[5], (NC, NC), NC ** -0.5, 0.21875, ((0, 16), (1, 2)), jnp.float32),
    }


HIGHEST = lax.Precision.HIGHEST


def reference(multipliers, own_modes, neighbour_modes, face_index, neighbour_list, coarse_factor):
    masked_modes = []
    for which_face in range(NFACE):
        masked_modes.append(neighbour_modes * (face_index == which_face).astype(jnp.float32)[None])
    coarse = jnp.einsum('ksm,rsm->krs', own_modes, multipliers, precision=HIGHEST)
    face_parts = []
    for which_face in range(NFACE):
        face_parts.append(jnp.einsum('ksm,rsm->krs', masked_modes[which_face], multipliers, precision=HIGHEST))
    face_terms = jnp.stack(face_parts, axis=3)
    flattened = face_terms.reshape(MODES, NRHS, NSUB * NFACE).transpose(2, 0, 1)
    targets = neighbour_list.reshape(NSUB * NFACE)
    incoming = jax.ops.segment_sum(flattened, targets, num_segments=NSUB)
    coarse = coarse + incoming.transpose(1, 2, 0)
    right_side = coarse.transpose(2, 0, 1).reshape(NSUB * MODES, NRHS)
    halfway = jnp.einsum('cp,cr->pr', coarse_factor, right_side, precision=HIGHEST)
    amplitudes = jnp.dot(coarse_factor, halfway, precision=HIGHEST, preferred_element_type=jnp.float32)
    amplitudes = amplitudes.reshape(NSUB, MODES, NRHS).transpose(1, 2, 0)
    applied = jnp.einsum('ksm,krs->rsm', own_modes, amplitudes, precision=HIGHEST)
    for which_face in range(NFACE):
        across = amplitudes[:, :, neighbour_list[:, which_face]]
        applied = applied + jnp.einsum('ksm,krs->rsm', masked_modes[which_face], across, precision=HIGHEST)
    return multipliers - applied
```

```python
import functools

import jax
import jax.numpy as jnp
from jax import lax
from jax.experimental import pallas as pl
from jax.experimental.pallas import tpu as pltpu
from jax.sharding import PartitionSpec as P

MESH = pl.DeviceIdType.MESH
NT = (((1,), (1,)), ((), ()))
NN = (((1,), (0,)), ((), ()))
LANES = 128
EDGE = 8


def each(count, step):
    if count <= 64:
        for i in range(count):
            step(i)
    else:
        lax.fori_loop(0, count, lambda i, t: (step(i), t)[1], 0)


def split(value):
    high = value.astype(jnp.bfloat16)
    return high, (value - high.astype(jnp.float32)).astype(jnp.bfloat16)


def dot3(left, right, dims):
    (lh, ll), (rh, rl) = left, right
    dot = functools.partial(
        lax.dot_general, dimension_numbers=dims, preferred_element_type=jnp.float32
    )
    return dot(lh, rh) + (dot(lh, rl) + dot(ll, rh))


def kernel(
    sub_size, crs_size,
    mult, own, nbr, face, nlist, factor, out,
    modes, c_send, c_recv, fcat, rs_send, rs_recv, ag_send, panel,
    c_ssem, c_rsem, f_ssem, f_rsem, rs_ssem, rs_rsem, ag_ssem, ag_rsem,
):
    nk, subs, width = own.shape
    nrhs = mult.shape[0]
    nface = nlist.shape[1]
    part = nk * subs
    parts = sub_size // nrhs
    row_len = sub_size // 2
    group = subs * crs_size
    devices = sub_size * crs_size
    g = lax.axis_index("sub")
    c = lax.axis_index("crs")
    me = g * crs_size + c
    up, down = part, part + EDGE
    off_x = part + 2 * EDGE
    off_n, off_p = off_x + part, off_x + 2 * part

    def rank(i):
        other = lax.rem(me + i, devices)
        return (other // crs_size, lax.rem(other, crs_size))

    barrier = pltpu.get_barrier_semaphore()
    each(devices - 1, lambda i: pl.semaphore_signal(
        barrier, inc=1, device_id=rank(i + 1), device_id_type=MESH))

    first, second = g // row_len, lax.rem(g, row_len)
    across = lax.rem(first + 1, 2) * row_len + second
    after = first * row_len + lax.rem(second + 1, row_len)
    before = first * row_len + lax.rem(second + row_len - 1, row_len)
    groups = (g, across, after, before)

    modes[...] = jnp.zeros_like(modes)
    fc = face[...]
    first_sub = me * subs
    names = nlist[pl.ds(first_sub, subs), :]
    target = jnp.zeros((subs, width), jnp.int32)
    for f in range(nface):
        target = jnp.where(fc == f, names[:, f:f + 1], target)
    third = c * subs + lax.broadcasted_iota(jnp.int32, (subs, width), 0)
    nxt = jnp.where(third == group - 1, 0, third + 1)
    prv = jnp.where(third == 0, group - 1, third - 1)

    def chosen(block, line):
        return jnp.where(target == block * group + line, 1.0, 0.0)

    masks = (
        chosen(g, nxt), chosen(g, prv),
        chosen(across, third), chosen(after, third), chosen(before, third),
    )
    for s in range(subs):
        cols = pl.ds(s * width, width)
        own_s = own[:, s, :]
        nbr_s = nbr[:, s, :]
        rows = (
            nk * (s + 1) if s < subs - 1 else up,
            nk * (s - 1) if s > 0 else down + EDGE - nk,
            off_x + nk * s, off_n + nk * s, off_p + nk * s,
        )
        modes[pl.ds(nk * s, nk), cols] = own_s
        for d in range(5):
            value = nbr_s * masks[d][s:s + 1, :]
            spot = pl.ds(rows[d], nk)
            modes[spot, cols] = value
    sums = jnp.zeros((nrhs, modes.shape[0]), jnp.float32)
    for s in range(subs):
        cols = pl.ds(s * width, width)
        sums = sums + dot3(split(mult[:, s, :]), split(modes[:, cols]), NT)
    c_send[:, :modes.shape[0]] = sums
    c_recv[0, c, :, :modes.shape[0]] = sums

    pl.semaphore_wait(barrier, devices - 1)

    def c_copy(j, i):
        to = lax.rem(c + i, crs_size)
        return pltpu.make_async_remote_copy(
            src_ref=c_send, dst_ref=c_recv.at[j, c],
            send_sem=c_ssem.at[j, i], recv_sem=c_rsem.at[j, i],
            device_id=(groups[j], to), device_id_type=MESH)

    def c_wait(j, i):
        src = lax.rem(c + crs_size - i, crs_size)
        pltpu.make_async_remote_copy(
            src_ref=c_send, dst_ref=c_recv.at[j, src],
            send_sem=c_ssem.at[j, i], recv_sem=c_rsem.at[j, i],
            device_id=(groups[j], src), device_id_type=MESH).wait_recv()

    for j in (1, 2, 3, 0):
        for i in range(crs_size):
            if j or i:
                c_copy(j, i).start()

    def row(p, extra=0):
        return pl.multiple_of(p * part + extra, 8)

    def f_pieces(i):
        to = lax.rem(c + i, crs_size)
        nx = lax.rem(to + 1, crs_size)
        pv = lax.rem(to + crs_size - 1, crs_size)
        return to, (
            (row(to), 0, part, g),
            (row(nx), up, EDGE, g),
            (row(pv, part - EDGE), down, EDGE, g),
            (row(to), off_x, part, across),
            (row(to), off_p, part, after),
            (row(to), off_n, part, before),
        )

    def f_copy(i, n):
        to, pieces = f_pieces(i)
        start, place, size, where = pieces[n]
        return pltpu.make_async_remote_copy(
            src_ref=factor.at[pl.ds(start, size), :],
            dst_ref=fcat.at[c, pl.ds(place, size), :],
            send_sem=f_ssem.at[i, n], recv_sem=f_rsem.at[i, n],
            device_id=(where, to), device_id_type=MESH)

    def f_wait(i, n):
        to, pieces = f_pieces(i)
        start, place, size, where = pieces[n]
        src = lax.rem(c + crs_size - i, crs_size)
        pltpu.make_async_remote_copy(
            src_ref=factor.at[pl.ds(start, size), :],
            dst_ref=fcat.at[src, pl.ds(place, size), :],
            send_sem=f_ssem.at[i, n], recv_sem=f_rsem.at[i, n],
            device_id=(where, to), device_id_type=MESH).wait_recv()

    moves = [(i, n) for i in range(crs_size) for n in range(6) if i or n > 2]
    for i, n in moves:
        f_copy(i, n).start()
    _, pieces = f_pieces(0)
    for start, place, size, _ in pieces[:3]:
        fcat[c, pl.ds(place, size), :] = factor[pl.ds(start, size), :]

    for j in (0, 1, 2, 3):
        for i in range(crs_size):
            if j or i:
                c_wait(j, i)

    lane = lax.broadcasted_iota(jnp.int32, (nrhs, LANES), 1)

    def rolled(value, by):
        return pltpu.roll(value, LANES - by, 1)

    total = jnp.zeros((nrhs, factor.shape[1]), jnp.float32)
    for p in range(crs_size):
        low = c_recv[0, (p - 1) % crs_size]
        high = c_recv[0, (p + 1) % crs_size]
        rhs = c_recv[0, p]
        rhs = rhs + jnp.where(lane < EDGE, rolled(low, up), 0.0)
        rhs = rhs + jnp.where(lane >= part - EDGE, rolled(high, down - (part - EDGE)), 0.0)
        rhs = rhs + rolled(c_recv[1, p], off_x)
        rhs = rhs + rolled(c_recv[2, p], off_n)
        rhs = rhs + rolled(c_recv[3, p], off_p)
        total = total + dot3(
            split(rhs[:, :part]), split(factor[p * part:(p + 1) * part, :]), NN)

    chunk = factor.shape[1] // parts
    for q in range(parts):
        for r in range(nrhs):
            rs_send[q * nrhs + r] = total[r:r + 1, q * chunk:(q + 1) * chunk]

    def rs_copy(i):
        to = lax.rem(g + i, sub_size)
        return pltpu.make_async_remote_copy(
            src_ref=rs_send.at[to], dst_ref=rs_recv.at[g],
            send_sem=rs_ssem.at[i], recv_sem=rs_rsem.at[i],
            device_id=(to, c), device_id_type=MESH)

    def rs_wait(i):
        src = lax.rem(g + sub_size - i, sub_size)
        pltpu.make_async_remote_copy(
            src_ref=rs_send.at[src], dst_ref=rs_recv.at[src],
            send_sem=rs_ssem.at[i], recv_sem=rs_rsem.at[i],
            device_id=(src, c), device_id_type=MESH).wait_recv()

    each(sub_size - 1, lambda i: rs_copy(i + 1).start())
    rs_recv[g] = rs_send[g]
    each(sub_size - 1, lambda i: rs_wait(i + 1))
    mine = rs_recv[0]
    for q in range(1, sub_size):
        mine = mine + rs_recv[q]
    ag_send[...] = mine

    def ag_copy(i):
        return pltpu.make_async_remote_copy(
            src_ref=ag_send, dst_ref=panel.at[c, g],
            send_sem=ag_ssem.at[i], recv_sem=ag_rsem.at[i],
            device_id=rank(i), device_id_type=MESH)

    def ag_wait(i):
        fg, fcr = rank(devices - i)
        pltpu.make_async_remote_copy(
            src_ref=ag_send, dst_ref=panel.at[fcr, fg],
            send_sem=ag_ssem.at[i], recv_sem=ag_rsem.at[i],
            device_id=(fg, fcr), device_id_type=MESH).wait_recv()

    each(devices - 1, lambda i: ag_copy(i + 1).start())
    panel[c, g] = mine
    for i, n in moves:
        f_wait(i, n)
    each(devices - 1, lambda i: ag_wait(i + 1))

    amps = jnp.zeros((nrhs, modes.shape[0]), jnp.float32)
    for p in range(crs_size):
        for q in range(parts):
            rows = panel[p, q * nrhs:(q + 1) * nrhs].reshape(nrhs, chunk)
            amps = amps + dot3(
                split(rows), split(fcat[p, :, q * chunk:(q + 1) * chunk]), NT)
    amps = split(amps)
    for s in range(subs):
        cols = pl.ds(s * width, width)
        out[:, s, :] = mult[:, s, :] - dot3(amps, split(modes[:, cols]), NN)

    for j in range(4):
        for i in range(crs_size):
            if j or i:
                c_copy(j, i).wait_send()
    for i, n in moves:
        f_copy(i, n).wait_send()
    each(sub_size - 1, lambda i: rs_copy(i + 1).wait_send())
    each(devices - 1, lambda i: ag_copy(i + 1).wait_send())


def body(sub_size, crs_size, mult, own, nbr, face, nlist, factor):
    nk, subs, width = own.shape
    nrhs = mult.shape[0]
    part = nk * subs
    frame = 4 * part + 2 * EDGE
    cols = factor.shape[1]
    chunk = cols * nrhs // sub_size
    f32 = jnp.float32
    dma = pltpu.SemaphoreType.DMA
    vmem = pl.BlockSpec(memory_space=pltpu.VMEM)
    return pl.pallas_call(
        functools.partial(kernel, sub_size, crs_size),
        out_shape=jax.ShapeDtypeStruct(mult.shape, mult.dtype),
        in_specs=[vmem] * 6,
        out_specs=vmem,
        scratch_shapes=[
            pltpu.VMEM((frame, subs * width), f32),
            pltpu.VMEM((nrhs, LANES), f32),
            pltpu.VMEM((4, crs_size, nrhs, LANES), f32),
            pltpu.VMEM((crs_size, frame, cols), f32),
            pltpu.VMEM((sub_size, 1, chunk), f32),
            pltpu.VMEM((sub_size, 1, chunk), f32),
            pltpu.VMEM((1, chunk), f32),
            pltpu.VMEM((crs_size, sub_size, 1, chunk), f32),
            dma((4, crs_size)), dma((4, crs_size)),
            dma((crs_size, 6)), dma((crs_size, 6)),
            dma((sub_size,)), dma((sub_size,)),
            dma((sub_size * crs_size,)), dma((sub_size * crs_size,)),
        ],
        compiler_params=pltpu.CompilerParams(collective_id=0, has_side_effects=True),
    )(mult, own, nbr, face, nlist, factor)


def solution(mesh):
    placed = (
        P(None, ("sub", "crs"), None),
        P(None, ("sub", "crs"), None),
        P(None, ("sub", "crs"), None),
        P(("sub", "crs"), None),
        P(),
        P("sub", "crs"),
    )
    return jax.shard_map(
        functools.partial(body, mesh.shape["sub"], mesh.shape["crs"]),
        mesh=mesh, in_specs=placed, out_specs=P(None, ("sub", "crs"), None), check_vma=False
    )
```

```python
import functools

import jax
import jax.numpy as jnp
from jax import lax
from jax.experimental import pallas as pl
from jax.experimental.pallas import tpu as pltpu
from jax.sharding import PartitionSpec as P

MESH = pl.DeviceIdType.MESH
NT = (((1,), (1,)), ((), ()))
NN = (((1,), (0,)), ((), ()))
LANES = 128
EDGE = 8


def each(count, step):
    if count <= 64:
        for i in range(count):
            step(i)
    else:
        lax.fori_loop(0, count, lambda i, t: (step(i), t)[1], 0)


def both(value, axis=0):
    high = value.astype(jnp.bfloat16)
    low = (value - high.astype(jnp.float32)).astype(jnp.bfloat16)
    return jnp.concatenate([high, low], axis=axis)


def halves(value):
    rows = value.shape[0] // 2
    return value[:rows] + value[rows:]


def quarters(value):
    value = halves(value)
    cols = value.shape[1] // 2
    return value[:, :cols] + value[:, cols:]


def dot(left, right, dims):
    return lax.dot_general(left, right, dims, preferred_element_type=jnp.float32)


def twice(left, right):
    high = left.astype(jnp.bfloat16)
    low = (left - high.astype(jnp.float32)).astype(jnp.bfloat16)
    wide = jnp.concatenate(
        [jnp.concatenate([high, high], axis=1), jnp.concatenate([low, low], axis=1)], axis=0)
    return halves(dot(wide, right, NN))


def kernel(
    sub_size, crs_size,
    mult_h, own_h, nbr_h, face_h, nlist_h, factor_h, out_h,
    mult, own, nbr, face, nlist, factor, out,
    modes, pair, c_send, c_recv, fcat, fown, fpair, rs_send, rs_recv, ag_send, panel,
    c_ssem, c_rsem, f_ssem, f_rsem, rs_ssem, rs_rsem, ag_ssem, ag_rsem, in_sem,
):
    nk, subs, width = own.shape
    nrhs = mult.shape[0]
    nface = nlist.shape[0]
    part = nk * subs
    parts = sub_size // nrhs
    row_len = sub_size // 2
    group = subs * crs_size
    devices = sub_size * crs_size
    g = lax.axis_index("sub")
    c = lax.axis_index("crs")
    me = g * crs_size + c
    up, down = part, part + EDGE
    off_x = part + 2 * EDGE
    off_n, off_p = off_x + part, off_x + 2 * part

    def rank(i):
        other = lax.rem(me + i, devices)
        return (other // crs_size, lax.rem(other, crs_size))

    loads = [
        pltpu.make_async_copy(a, b, in_sem.at[i]) for i, (a, b) in enumerate((
            (nlist_h, nlist), (face_h, face), (nbr_h, nbr), (own_h, own),
            (mult_h, mult), (factor_h, factor)))
    ]
    for load in loads:
        load.start()
    barrier = pltpu.get_barrier_semaphore()
    each(devices - 1, lambda i: pl.semaphore_signal(
        barrier, inc=1, device_id=rank(i + 1), device_id_type=MESH))

    first, second = g // row_len, lax.rem(g, row_len)
    across = lax.rem(first + 1, 2) * row_len + second
    after = first * row_len + lax.rem(second + 1, row_len)
    before = first * row_len + lax.rem(second + row_len - 1, row_len)
    groups = (g, across, after, before)

    modes[...] = jnp.zeros_like(modes)
    fcat[:, down + EDGE + 3 * part:, :] = jnp.zeros(
        (crs_size, LANES - (down + EDGE + 3 * part), fcat.shape[2]), jnp.float32)
    for load in loads[:4]:
        load.wait()
    fc = face[...]
    first_sub = me * subs
    line = lax.broadcasted_iota(jnp.int32, (subs, width), 0)
    target = jnp.zeros((subs, width), jnp.int32)
    for f in range(nface):
        name = jnp.zeros((subs, width), jnp.int32)
        for s in range(subs):
            name = jnp.where(line == s, nlist[f, first_sub + s], name)
        target = jnp.where(fc == f, name, target)
    third = c * subs + line
    nxt = jnp.where(third == group - 1, 0, third + 1)
    prv = jnp.where(third == 0, group - 1, third - 1)

    def chosen(block, line):
        return jnp.where(target == block * group + line, 1.0, 0.0)

    masks = (
        chosen(g, nxt), chosen(g, prv),
        chosen(across, third), chosen(after, third), chosen(before, third),
    )
    for s in range(subs):
        cols = pl.ds(s * width, width)
        own_s = own[:, s, :]
        nbr_s = nbr[:, s, :]
        rows = (
            nk * (s + 1) if s < subs - 1 else up,
            nk * (s - 1) if s > 0 else down + EDGE - nk,
            off_x + nk * s, off_n + nk * s, off_p + nk * s,
        )
        modes[pl.ds(nk * s, nk), cols] = own_s
        for d in range(5):
            value = nbr_s * masks[d][s:s + 1, :]
            spot = pl.ds(rows[d], nk)
            modes[spot, cols] = value
    pair[...] = both(modes[...])
    loads[4].wait()
    sums = jnp.zeros((2 * nrhs, 2 * LANES), jnp.float32)
    for s in range(subs):
        cols = pl.ds(s * width, width)
        sums = sums + dot(both(mult[:, s, :]), pair[:, cols], NT)
    sums = quarters(sums)
    c_send[...] = sums
    c_recv[0, c] = sums

    pl.semaphore_wait(barrier, devices - 1)

    def c_copy(j, i):
        to = lax.rem(c + i, crs_size)
        return pltpu.make_async_remote_copy(
            src_ref=c_send, dst_ref=c_recv.at[j, c],
            send_sem=c_ssem.at[j, i], recv_sem=c_rsem.at[j, i],
            device_id=(groups[j], to), device_id_type=MESH)

    def c_wait(j, i):
        src = lax.rem(c + crs_size - i, crs_size)
        pltpu.make_async_remote_copy(
            src_ref=c_send, dst_ref=c_recv.at[j, src],
            send_sem=c_ssem.at[j, i], recv_sem=c_rsem.at[j, i],
            device_id=(groups[j], src), device_id_type=MESH).wait_recv()

    for j in (1, 2, 3, 0):
        for i in range(crs_size):
            if j or i:
                c_copy(j, i).start()

    def row(p, extra=0):
        return pl.multiple_of(p * part + extra, 8)

    def f_pieces(i):
        to = lax.rem(c + i, crs_size)
        nx = lax.rem(to + 1, crs_size)
        pv = lax.rem(to + crs_size - 1, crs_size)
        return to, (
            (row(to), 0, part, g),
            (row(nx), up, EDGE, g),
            (row(pv, part - EDGE), down, EDGE, g),
            (row(to), off_x, part, across),
            (row(to), off_p, part, after),
            (row(to), off_n, part, before),
        )

    def f_copy(i, n):
        to, pieces = f_pieces(i)
        start, place, size, where = pieces[n]
        return pltpu.make_async_remote_copy(
            src_ref=factor.at[pl.ds(start, size), :],
            dst_ref=fcat.at[c, pl.ds(place, size), :],
            send_sem=f_ssem.at[i, n], recv_sem=f_rsem.at[i, n],
            device_id=(where, to), device_id_type=MESH)

    def f_wait(i, n):
        to, pieces = f_pieces(i)
        start, place, size, where = pieces[n]
        src = lax.rem(c + crs_size - i, crs_size)
        pltpu.make_async_remote_copy(
            src_ref=factor.at[pl.ds(start, size), :],
            dst_ref=fcat.at[src, pl.ds(place, size), :],
            send_sem=f_ssem.at[i, n], recv_sem=f_rsem.at[i, n],
            device_id=(where, to), device_id_type=MESH).wait_recv()

    loads[5].wait()
    span = LANES // part
    blocks = fown.shape[0]
    for b in range(blocks):
        held = factor[b * span * part:min((b + 1) * span, crs_size) * part, :]
        if held.shape[0] < LANES:
            held = jnp.concatenate(
                [held, jnp.zeros((LANES - held.shape[0], held.shape[1]), jnp.float32)], axis=0)
        fown[b] = both(held)

    for j in (0, 1, 2, 3):
        for i in range(crs_size):
            if j or i:
                c_wait(j, i)

    lane = lax.broadcasted_iota(jnp.int32, (nrhs, LANES), 1)

    def rolled(value, by):
        return pltpu.roll(value, (LANES - by) % LANES, 1) if by % LANES else value

    total = jnp.zeros((nrhs, factor.shape[1]), jnp.float32)
    for b in range(blocks):
        group_rhs = jnp.zeros((nrhs, LANES), jnp.float32)
        for p in range(b * span, min((b + 1) * span, crs_size)):
            at = (p - b * span) * part
            low = c_recv[0, (p - 1) % crs_size]
            high = c_recv[0, (p + 1) % crs_size]
            rhs = rolled(c_recv[0, p], -at)
            rhs = rhs + jnp.where(lane < at + EDGE, rolled(low, up - at), 0.0)
            rhs = rhs + jnp.where(
                lane >= at + part - EDGE, rolled(high, down - (at + part - EDGE)), 0.0)
            rhs = rhs + rolled(c_recv[1, p], off_x - at)
            rhs = rhs + rolled(c_recv[2, p], off_n - at)
            rhs = rhs + rolled(c_recv[3, p], off_p - at)
            group_rhs = jnp.where((lane >= at) & (lane < at + part), rhs, group_rhs)
        total = total + twice(group_rhs, fown[b])

    chunk = factor.shape[1] // parts
    for q in range(parts):
        for r in range(nrhs):
            rs_send[q * nrhs + r] = total[r:r + 1, q * chunk:(q + 1) * chunk]

    def rs_copy(i):
        to = lax.rem(g + i, sub_size)
        return pltpu.make_async_remote_copy(
            src_ref=rs_send.at[to], dst_ref=rs_recv.at[g],
            send_sem=rs_ssem.at[i], recv_sem=rs_rsem.at[i],
            device_id=(to, c), device_id_type=MESH)

    def rs_wait(i):
        src = lax.rem(g + sub_size - i, sub_size)
        pltpu.make_async_remote_copy(
            src_ref=rs_send.at[src], dst_ref=rs_recv.at[src],
            send_sem=rs_ssem.at[i], recv_sem=rs_rsem.at[i],
            device_id=(src, c), device_id_type=MESH).wait_recv()

    each(sub_size - 1, lambda i: rs_copy(i + 1).start())
    moves = [(i, n) for i in range(crs_size) for n in range(6) if i or n > 2]
    for i, n in moves:
        f_copy(i, n).start()
    _, pieces = f_pieces(0)
    for start, place, size, _ in pieces[:3]:
        fcat[c, pl.ds(place, size), :] = factor[pl.ds(start, size), :]

    rs_recv[g] = rs_send[g]
    each(sub_size - 1, lambda i: rs_wait(i + 1))
    mine = rs_recv[0]
    for q in range(1, sub_size):
        mine = mine + rs_recv[q]
    ag_send[...] = mine

    def ag_copy(i):
        return pltpu.make_async_remote_copy(
            src_ref=ag_send, dst_ref=panel.at[c, g],
            send_sem=ag_ssem.at[i], recv_sem=ag_rsem.at[i],
            device_id=rank(i), device_id_type=MESH)

    def ag_wait(i):
        fg, fcr = rank(devices - i)
        pltpu.make_async_remote_copy(
            src_ref=ag_send, dst_ref=panel.at[fcr, fg],
            send_sem=ag_ssem.at[i], recv_sem=ag_rsem.at[i],
            device_id=(fg, fcr), device_id_type=MESH).wait_recv()

    each(devices - 1, lambda i: ag_copy(i + 1).start())
    panel[c, g] = mine
    for i, n in moves:
        f_wait(i, n)
    for p in range(crs_size):
        fpair[p] = both(fcat[p])
    each(devices - 1, lambda i: ag_wait(i + 1))

    amps = jnp.zeros((2 * nrhs, 2 * LANES), jnp.float32)
    for p in range(crs_size):
        for q in range(parts):
            rows = panel[p, q * nrhs:(q + 1) * nrhs].reshape(nrhs, chunk)
            amps = amps + dot(both(rows), fpair[p, :, q * chunk:(q + 1) * chunk], NT)
    amps = quarters(amps)
    for s in range(subs):
        out[:, s, :] = mult[:, s, :] - twice(amps, pair[:, s * width:(s + 1) * width])
    store = pltpu.make_async_copy(out, out_h, in_sem.at[0])
    store.start()

    for j in range(4):
        for i in range(crs_size):
            if j or i:
                c_copy(j, i).wait_send()
    for i, n in moves:
        f_copy(i, n).wait_send()
    each(sub_size - 1, lambda i: rs_copy(i + 1).wait_send())
    each(devices - 1, lambda i: ag_copy(i + 1).wait_send())

    store.wait()


def body(sub_size, crs_size, mult, own, nbr, face, nlist, factor):
    nk, subs, width = own.shape
    nrhs = mult.shape[0]
    part = nk * subs
    blocks = -(-crs_size // (LANES // part))
    cols = factor.shape[1]
    chunk = cols * nrhs // sub_size
    f32 = jnp.float32
    dma = pltpu.SemaphoreType.DMA
    bf16 = jnp.bfloat16
    hbm = pl.BlockSpec(memory_space=pl.ANY)
    names = nlist.T
    return pl.pallas_call(
        functools.partial(kernel, sub_size, crs_size),
        out_shape=jax.ShapeDtypeStruct(mult.shape, mult.dtype),
        in_specs=[hbm] * 6,
        out_specs=hbm,
        scratch_shapes=[
            pltpu.VMEM(mult.shape, f32), pltpu.VMEM(own.shape, f32), pltpu.VMEM(nbr.shape, f32),
            pltpu.VMEM(face.shape, face.dtype), pltpu.SMEM(names.shape, names.dtype),
            pltpu.VMEM(factor.shape, f32), pltpu.VMEM(mult.shape, f32),
            pltpu.VMEM((LANES, subs * width), f32),
            pltpu.VMEM((2 * LANES, subs * width), bf16),
            pltpu.VMEM((nrhs, LANES), f32),
            pltpu.VMEM((4, crs_size, nrhs, LANES), f32),
            pltpu.VMEM((crs_size, LANES, cols), f32),
            pltpu.VMEM((blocks, 2 * LANES, cols), bf16),
            pltpu.VMEM((crs_size, 2 * LANES, cols), bf16),
            pltpu.VMEM((sub_size, 1, chunk), f32),
            pltpu.VMEM((sub_size, 1, chunk), f32),
            pltpu.VMEM((1, chunk), f32),
            pltpu.VMEM((crs_size, sub_size, 1, chunk), f32),
            dma((4, crs_size)), dma((4, crs_size)),
            dma((crs_size, 6)), dma((crs_size, 6)),
            dma((sub_size,)), dma((sub_size,)),
            dma((sub_size * crs_size,)), dma((sub_size * crs_size,)), dma((6,)),
        ],
        compiler_params=pltpu.CompilerParams(collective_id=0, has_side_effects=True),
    )(mult, own, nbr, face, names, factor)


def solution(mesh):
    placed = (
        P(None, ("sub", "crs"), None),
        P(None, ("sub", "crs"), None),
        P(None, ("sub", "crs"), None),
        P(("sub", "crs"), None),
        P(),
        P("sub", "crs"),
    )
    return jax.shard_map(
        functools.partial(body, mesh.shape["sub"], mesh.shape["crs"]),
        mesh=mesh, in_specs=placed, out_specs=P(None, ("sub", "crs"), None), check_vma=False
    )
```

```python
import functools

import jax
import jax.numpy as jnp
from jax import lax
from jax.experimental import pallas as pl
from jax.experimental.pallas import tpu as pltpu
from jax.sharding import PartitionSpec as P

MESH = pl.DeviceIdType.MESH
NT = (((1,), (1,)), ((), ()))
NN = (((1,), (0,)), ((), ()))
LANES = 128
EDGE = 8


def each(count, step):
    if count <= 64:
        for i in range(count):
            step(i)
    else:
        lax.fori_loop(0, count, lambda i, t: (step(i), t)[1], 0)


def both(value, axis=0):
    high = value.astype(jnp.bfloat16)
    low = (value - high.astype(jnp.float32)).astype(jnp.bfloat16)
    return jnp.concatenate([high, low], axis=axis)


def halves(value):
    rows = value.shape[0] // 2
    return value[:rows] + value[rows:]


def quarters(value):
    value = halves(value)
    cols = value.shape[1] // 2
    return value[:, :cols] + value[:, cols:]


def dot(left, right, dims):
    return lax.dot_general(left, right, dims, preferred_element_type=jnp.float32)


def twice(left, right):
    high = left.astype(jnp.bfloat16)
    low = (left - high.astype(jnp.float32)).astype(jnp.bfloat16)
    wide = jnp.concatenate(
        [jnp.concatenate([high, high], axis=1), jnp.concatenate([low, low], axis=1)], axis=0)
    return halves(dot(wide, right, NN))


def kernel(
    sub_size, crs_size,
    mult_h, own_h, nbr_h, face_h, nlist_h, factor_h, out_h,
    mult, own, nbr, face, nlist, factor, out,
    modes, pair, c_send, c_recv, fcat, fown, fpair, rs_send, rs_recv, ag_send, panel,
    c_ssem, c_rsem, f_ssem, f_rsem, rs_ssem, rs_rsem, ag_ssem, ag_rsem, in_sem, met,
):
    nk, subs, width = own.shape
    nrhs = mult.shape[0]
    nface = nlist.shape[0]
    part = nk * subs
    parts = sub_size // nrhs
    row_len = sub_size // 2
    group = subs * crs_size
    devices = sub_size * crs_size
    g = lax.axis_index("sub")
    c = lax.axis_index("crs")
    me = g * crs_size + c
    up, down = part, part + EDGE
    off_x = part + 2 * EDGE
    off_n, off_p = off_x + part, off_x + 2 * part

    def rank(i):
        other = lax.rem(me + i, devices)
        return (other // crs_size, lax.rem(other, crs_size))

    loads = [
        pltpu.make_async_copy(a, b, in_sem.at[i]) for i, (a, b) in enumerate((
            (nlist_h, nlist), (face_h, face), (nbr_h, nbr), (own_h, own),
            (mult_h, mult), (factor_h, factor)))
    ]
    for load in loads:
        load.start()
    barrier = pltpu.get_barrier_semaphore()
    first, second = g // row_len, lax.rem(g, row_len)
    across = lax.rem(first + 1, 2) * row_len + second
    after = first * row_len + lax.rem(second + 1, row_len)
    before = first * row_len + lax.rem(second + row_len - 1, row_len)
    groups = (g, across, after, before)

    block = 1 << (devices.bit_length() // 2)
    base = me // block * block
    inner = [base + lax.rem(me - base + i, block) for i in range(1, block)]
    outer = [lax.rem(me + i, devices) for i in range(block, devices, block)]
    near = [groups[j] * crs_size + lax.rem(c + i, crs_size)
            for j in range(4) for i in range(crs_size) if j or i]

    def signal(semaphore, other):
        pl.semaphore_signal(
            semaphore, inc=1, device_id=(other // crs_size, lax.rem(other, crs_size)),
            device_id_type=MESH)

    for other in outer + near + inner:
        signal(barrier, other)

    modes[...] = jnp.zeros_like(modes)
    fcat[:, down + EDGE + 3 * part:, :] = jnp.zeros(
        (crs_size, LANES - (down + EDGE + 3 * part), fcat.shape[2]), jnp.float32)
    for load in loads[:4]:
        load.wait()
    fc = face[...]
    first_sub = me * subs
    line = lax.broadcasted_iota(jnp.int32, (subs, width), 0)
    target = jnp.zeros((subs, width), jnp.int32)
    for f in range(nface):
        name = jnp.zeros((subs, width), jnp.int32)
        for s in range(subs):
            name = jnp.where(line == s, nlist[f, first_sub + s], name)
        target = jnp.where(fc == f, name, target)
    third = c * subs + line
    nxt = jnp.where(third == group - 1, 0, third + 1)
    prv = jnp.where(third == 0, group - 1, third - 1)

    def chosen(block, line):
        return jnp.where(target == block * group + line, 1.0, 0.0)

    masks = (
        chosen(g, nxt), chosen(g, prv),
        chosen(across, third), chosen(after, third), chosen(before, third),
    )
    for s in range(subs):
        cols = pl.ds(s * width, width)
        own_s = own[:, s, :]
        nbr_s = nbr[:, s, :]
        rows = (
            nk * (s + 1) if s < subs - 1 else up,
            nk * (s - 1) if s > 0 else down + EDGE - nk,
            off_x + nk * s, off_n + nk * s, off_p + nk * s,
        )
        modes[pl.ds(nk * s, nk), cols] = own_s
        for d in range(5):
            value = nbr_s * masks[d][s:s + 1, :]
            spot = pl.ds(rows[d], nk)
            modes[spot, cols] = value
    pair[...] = both(modes[...])
    loads[4].wait()
    sums = jnp.zeros((2 * nrhs, 2 * LANES), jnp.float32)
    for s in range(subs):
        cols = pl.ds(s * width, width)
        sums = sums + dot(both(mult[:, s, :]), pair[:, cols], NT)
    sums = quarters(sums)
    c_send[...] = sums
    c_recv[0, c] = sums

    pl.semaphore_wait(barrier, len(outer) + len(near) + len(inner))

    def c_copy(j, i):
        to = lax.rem(c + i, crs_size)
        return pltpu.make_async_remote_copy(
            src_ref=c_send, dst_ref=c_recv.at[j, c],
            send_sem=c_ssem.at[j, i], recv_sem=c_rsem.at[j, i],
            device_id=(groups[j], to), device_id_type=MESH)

    def c_wait(j, i):
        src = lax.rem(c + crs_size - i, crs_size)
        pltpu.make_async_remote_copy(
            src_ref=c_send, dst_ref=c_recv.at[j, src],
            send_sem=c_ssem.at[j, i], recv_sem=c_rsem.at[j, i],
            device_id=(groups[j], src), device_id_type=MESH).wait_recv()

    for j in (1, 2, 3, 0):
        for i in range(crs_size):
            if j or i:
                c_copy(j, i).start()

    def row(p, extra=0):
        return pl.multiple_of(p * part + extra, 8)

    def f_pieces(i):
        to = lax.rem(c + i, crs_size)
        nx = lax.rem(to + 1, crs_size)
        pv = lax.rem(to + crs_size - 1, crs_size)
        return to, (
            (row(to), 0, part, g),
            (row(nx), up, EDGE, g),
            (row(pv, part - EDGE), down, EDGE, g),
            (row(to), off_x, part, across),
            (row(to), off_p, part, after),
            (row(to), off_n, part, before),
        )

    def f_copy(i, n):
        to, pieces = f_pieces(i)
        start, place, size, where = pieces[n]
        return pltpu.make_async_remote_copy(
            src_ref=factor.at[pl.ds(start, size), :],
            dst_ref=fcat.at[c, pl.ds(place, size), :],
            send_sem=f_ssem.at[i, n], recv_sem=f_rsem.at[i, n],
            device_id=(where, to), device_id_type=MESH)

    def f_wait(i, n):
        to, pieces = f_pieces(i)
        start, place, size, where = pieces[n]
        src = lax.rem(c + crs_size - i, crs_size)
        pltpu.make_async_remote_copy(
            src_ref=factor.at[pl.ds(start, size), :],
            dst_ref=fcat.at[src, pl.ds(place, size), :],
            send_sem=f_ssem.at[i, n], recv_sem=f_rsem.at[i, n],
            device_id=(where, to), device_id_type=MESH).wait_recv()

    for other in outer:
        signal(met, other)

    loads[5].wait()
    span = LANES // part
    blocks = fown.shape[0]
    for b in range(blocks):
        held = factor[b * span * part:min((b + 1) * span, crs_size) * part, :]
        if held.shape[0] < LANES:
            held = jnp.concatenate(
                [held, jnp.zeros((LANES - held.shape[0], held.shape[1]), jnp.float32)], axis=0)
        fown[b] = both(held)

    for j in (0, 1, 2, 3):
        for i in range(crs_size):
            if j or i:
                c_wait(j, i)

    lane = lax.broadcasted_iota(jnp.int32, (nrhs, LANES), 1)

    def rolled(value, by):
        return pltpu.roll(value, (LANES - by) % LANES, 1) if by % LANES else value

    total = jnp.zeros((nrhs, factor.shape[1]), jnp.float32)
    for b in range(blocks):
        group_rhs = jnp.zeros((nrhs, LANES), jnp.float32)
        for p in range(b * span, min((b + 1) * span, crs_size)):
            at = (p - b * span) * part
            low = c_recv[0, (p - 1) % crs_size]
            high = c_recv[0, (p + 1) % crs_size]
            rhs = rolled(c_recv[0, p], -at)
            rhs = rhs + jnp.where(lane < at + EDGE, rolled(low, up - at), 0.0)
            rhs = rhs + jnp.where(
                lane >= at + part - EDGE, rolled(high, down - (at + part - EDGE)), 0.0)
            rhs = rhs + rolled(c_recv[1, p], off_x - at)
            rhs = rhs + rolled(c_recv[2, p], off_n - at)
            rhs = rhs + rolled(c_recv[3, p], off_p - at)
            group_rhs = jnp.where((lane >= at) & (lane < at + part), rhs, group_rhs)
        total = total + twice(group_rhs, fown[b])

    chunk = factor.shape[1] // parts
    for q in range(parts):
        for r in range(nrhs):
            rs_send[q * nrhs + r] = total[r:r + 1, q * chunk:(q + 1) * chunk]

    def rs_copy(i):
        to = lax.rem(g + i, sub_size)
        return pltpu.make_async_remote_copy(
            src_ref=rs_send.at[to], dst_ref=rs_recv.at[g],
            send_sem=rs_ssem.at[i], recv_sem=rs_rsem.at[i],
            device_id=(to, c), device_id_type=MESH)

    def rs_wait(i):
        src = lax.rem(g + sub_size - i, sub_size)
        pltpu.make_async_remote_copy(
            src_ref=rs_send.at[src], dst_ref=rs_recv.at[src],
            send_sem=rs_ssem.at[i], recv_sem=rs_rsem.at[i],
            device_id=(src, c), device_id_type=MESH).wait_recv()

    pl.semaphore_wait(met, len(outer))
    each(sub_size - 1, lambda i: rs_copy(i + 1).start())
    moves = [(i, n) for i in range(crs_size) for n in range(6) if i or n > 2]
    for i, n in moves:
        f_copy(i, n).start()
    _, pieces = f_pieces(0)
    for start, place, size, _ in pieces[:3]:
        fcat[c, pl.ds(place, size), :] = factor[pl.ds(start, size), :]

    rs_recv[g] = rs_send[g]
    each(sub_size - 1, lambda i: rs_wait(i + 1))
    mine = rs_recv[0]
    for q in range(1, sub_size):
        mine = mine + rs_recv[q]
    ag_send[...] = mine

    def ag_copy(i):
        return pltpu.make_async_remote_copy(
            src_ref=ag_send, dst_ref=panel.at[c, g],
            send_sem=ag_ssem.at[i], recv_sem=ag_rsem.at[i],
            device_id=rank(i), device_id_type=MESH)

    def ag_wait(i):
        fg, fcr = rank(devices - i)
        pltpu.make_async_remote_copy(
            src_ref=ag_send, dst_ref=panel.at[fcr, fg],
            send_sem=ag_ssem.at[i], recv_sem=ag_rsem.at[i],
            device_id=(fg, fcr), device_id_type=MESH).wait_recv()

    each(devices - 1, lambda i: ag_copy(i + 1).start())
    panel[c, g] = mine
    for i, n in moves:
        f_wait(i, n)
    for p in range(crs_size):
        fpair[p] = both(fcat[p])
    each(devices - 1, lambda i: ag_wait(i + 1))

    amps = jnp.zeros((2 * nrhs, 2 * LANES), jnp.float32)
    for p in range(crs_size):
        for q in range(parts):
            rows = panel[p, q * nrhs:(q + 1) * nrhs].reshape(nrhs, chunk)
            amps = amps + dot(both(rows), fpair[p, :, q * chunk:(q + 1) * chunk], NT)
    amps = quarters(amps)
    for s in range(subs):
        out[:, s, :] = mult[:, s, :] - twice(amps, pair[:, s * width:(s + 1) * width])
    store = pltpu.make_async_copy(out, out_h, in_sem.at[0])
    store.start()

    for j in range(4):
        for i in range(crs_size):
            if j or i:
                c_copy(j, i).wait_send()
    for i, n in moves:
        f_copy(i, n).wait_send()
    each(sub_size - 1, lambda i: rs_copy(i + 1).wait_send())
    each(devices - 1, lambda i: ag_copy(i + 1).wait_send())

    store.wait()


def body(sub_size, crs_size, mult, own, nbr, face, nlist, factor):
    nk, subs, width = own.shape
    nrhs = mult.shape[0]
    part = nk * subs
    blocks = -(-crs_size // (LANES // part))
    cols = factor.shape[1]
    chunk = cols * nrhs // sub_size
    f32 = jnp.float32
    dma = pltpu.SemaphoreType.DMA
    bf16 = jnp.bfloat16
    hbm = pl.BlockSpec(memory_space=pl.ANY)
    names = nlist.T
    return pl.pallas_call(
        functools.partial(kernel, sub_size, crs_size),
        out_shape=jax.ShapeDtypeStruct(mult.shape, mult.dtype),
        in_specs=[hbm] * 6,
        out_specs=hbm,
        scratch_shapes=[
            pltpu.VMEM(mult.shape, f32), pltpu.VMEM(own.shape, f32), pltpu.VMEM(nbr.shape, f32),
            pltpu.VMEM(face.shape, face.dtype), pltpu.SMEM(names.shape, names.dtype),
            pltpu.VMEM(factor.shape, f32), pltpu.VMEM(mult.shape, f32),
            pltpu.VMEM((LANES, subs * width), f32),
            pltpu.VMEM((2 * LANES, subs * width), bf16),
            pltpu.VMEM((nrhs, LANES), f32),
            pltpu.VMEM((4, crs_size, nrhs, LANES), f32),
            pltpu.VMEM((crs_size, LANES, cols), f32),
            pltpu.VMEM((blocks, 2 * LANES, cols), bf16),
            pltpu.VMEM((crs_size, 2 * LANES, cols), bf16),
            pltpu.VMEM((sub_size, 1, chunk), f32),
            pltpu.VMEM((sub_size, 1, chunk), f32),
            pltpu.VMEM((1, chunk), f32),
            pltpu.VMEM((crs_size, sub_size, 1, chunk), f32),
            dma((4, crs_size)), dma((4, crs_size)),
            dma((crs_size, 6)), dma((crs_size, 6)),
            dma((sub_size,)), dma((sub_size,)),
            dma((sub_size * crs_size,)), dma((sub_size * crs_size,)), dma((6,)),
            pltpu.SemaphoreType.REGULAR,
        ],
        compiler_params=pltpu.CompilerParams(collective_id=0, has_side_effects=True),
    )(mult, own, nbr, face, names, factor)


def solution(mesh):
    placed = (
        P(None, ("sub", "crs"), None),
        P(None, ("sub", "crs"), None),
        P(None, ("sub", "crs"), None),
        P(("sub", "crs"), None),
        P(),
        P("sub", "crs"),
    )
    return jax.shard_map(
        functools.partial(body, mesh.shape["sub"], mesh.shape["crs"]),
        mesh=mesh, in_specs=placed, out_specs=P(None, ("sub", "crs"), None), check_vma=False
    )
```

```python
import functools

import jax
import jax.numpy as jnp
from jax import lax
from jax.experimental import pallas as pl
from jax.experimental.pallas import tpu as pltpu
from jax.sharding import PartitionSpec as P

MESH = pl.DeviceIdType.MESH
NT = (((1,), (1,)), ((), ()))
NN = (((1,), (0,)), ((), ()))
LANES = 128
EDGE = 8


def each(count, step):
    if count <= 64:
        for i in sorted(range(count), key=lambda i: min(i, count - 1 - i)):
            step(i)
    else:
        lax.fori_loop(0, count, lambda i, t: (step(i), t)[1], 0)


def both(value, axis=0):
    high = value.astype(jnp.bfloat16)
    low = (value - high.astype(jnp.float32)).astype(jnp.bfloat16)
    return jnp.concatenate([high, low], axis=axis)


def halves(value):
    rows = value.shape[0] // 2
    return value[:rows] + value[rows:]


def quarters(value):
    value = halves(value)
    cols = value.shape[1] // 2
    return value[:, :cols] + value[:, cols:]


def dot(left, right, dims):
    return lax.dot_general(left, right, dims, preferred_element_type=jnp.float32)


def twice(left, right):
    high = left.astype(jnp.bfloat16)
    low = (left - high.astype(jnp.float32)).astype(jnp.bfloat16)
    wide = jnp.concatenate(
        [jnp.concatenate([high, high], axis=1), jnp.concatenate([low, low], axis=1)], axis=0)
    return halves(dot(wide, right, NN))


def kernel(
    sub_size, crs_size,
    mult_h, own_h, nbr_h, face_h, nlist_h, factor_h, out_h,
    mult, own, nbr, face, nlist, factor,
    modes, pair, c_send, c_recv, fcat, fown, fpair, rs_send, rs_recv, ag_send, panel,
    c_ssem, c_rsem, f_ssem, f_rsem, rs_ssem, rs_rsem, ag_ssem, ag_rsem, in_sem, met,
):
    nk, subs, width = own.shape
    nrhs = mult.shape[0]
    nface = nlist.shape[0]
    part = nk * subs
    parts = sub_size // nrhs
    row_len = sub_size // 2
    group = subs * crs_size
    devices = sub_size * crs_size
    g = lax.axis_index("sub")
    c = lax.axis_index("crs")
    me = g * crs_size + c
    up, down = part, part + EDGE
    off_x = part + 2 * EDGE
    off_n, off_p = off_x + part, off_x + 2 * part

    def rank(i):
        other = lax.rem(me + i, devices)
        return (other // crs_size, lax.rem(other, crs_size))

    loads = [
        pltpu.make_async_copy(a, b, in_sem.at[i]) for i, (a, b) in enumerate((
            (nlist_h, nlist), (face_h, face), (nbr_h, nbr), (own_h, own),
            (mult_h, mult), (factor_h, factor)))
    ]
    for load in loads:
        load.start()
    barrier = pltpu.get_barrier_semaphore()
    first, second = g // row_len, lax.rem(g, row_len)
    across = lax.rem(first + 1, 2) * row_len + second
    after = first * row_len + lax.rem(second + 1, row_len)
    before = first * row_len + lax.rem(second + row_len - 1, row_len)
    groups = (g, across, after, before)

    block = 1 << (devices.bit_length() // 2)
    base = me // block * block
    inner = [base + lax.rem(me - base + i, block) for i in range(1, block)]
    outer = [lax.rem(me + i, devices) for i in range(block, devices, block)]
    near = [groups[j] * crs_size + lax.rem(c + i, crs_size)
            for j in range(4) for i in range(crs_size) if j or i]

    def signal(semaphore, other):
        pl.semaphore_signal(
            semaphore, inc=1, device_id=(other // crs_size, lax.rem(other, crs_size)),
            device_id_type=MESH)

    for other in outer + near + inner:
        signal(barrier, other)

    modes[...] = jnp.zeros_like(modes)
    fcat[:, down + EDGE + 3 * part:, :] = jnp.zeros(
        (crs_size, LANES - (down + EDGE + 3 * part), fcat.shape[2]), jnp.float32)
    for load in loads[:4]:
        load.wait()
    fc = face[...]
    first_sub = me * subs
    line = lax.broadcasted_iota(jnp.int32, (subs, width), 0)
    target = jnp.zeros((subs, width), jnp.int32)
    for f in range(nface):
        name = jnp.zeros((subs, width), jnp.int32)
        for s in range(subs):
            name = jnp.where(line == s, nlist[f, first_sub + s], name)
        target = jnp.where(fc == f, name, target)
    third = c * subs + line
    nxt = jnp.where(third == group - 1, 0, third + 1)
    prv = jnp.where(third == 0, group - 1, third - 1)

    def chosen(block, line):
        return jnp.where(target == block * group + line, 1.0, 0.0)

    masks = (
        chosen(g, nxt), chosen(g, prv),
        chosen(across, third), chosen(after, third), chosen(before, third),
    )
    for s in range(subs):
        cols = pl.ds(s * width, width)
        own_s = own[:, s, :]
        nbr_s = nbr[:, s, :]
        rows = (
            nk * (s + 1) if s < subs - 1 else up,
            nk * (s - 1) if s > 0 else down + EDGE - nk,
            off_x + nk * s, off_n + nk * s, off_p + nk * s,
        )
        modes[pl.ds(nk * s, nk), cols] = own_s
        for d in range(5):
            value = nbr_s * masks[d][s:s + 1, :]
            spot = pl.ds(rows[d], nk)
            modes[spot, cols] = value
    pair[...] = both(modes[...])
    loads[4].wait()
    sums = jnp.zeros((2 * nrhs, 2 * LANES), jnp.float32)
    for s in range(subs):
        cols = pl.ds(s * width, width)
        sums = sums + dot(both(mult[:, s, :]), pair[:, cols], NT)
    sums = quarters(sums)
    c_send[...] = sums
    c_recv[0, c] = sums

    pl.semaphore_wait(barrier, len(outer) + len(near) + len(inner))

    def c_copy(j, i):
        to = lax.rem(c + i, crs_size)
        return pltpu.make_async_remote_copy(
            src_ref=c_send, dst_ref=c_recv.at[j, c],
            send_sem=c_ssem.at[j, i], recv_sem=c_rsem.at[j, i],
            device_id=(groups[j], to), device_id_type=MESH)

    def c_wait(j, i):
        src = lax.rem(c + crs_size - i, crs_size)
        pltpu.make_async_remote_copy(
            src_ref=c_send, dst_ref=c_recv.at[j, src],
            send_sem=c_ssem.at[j, i], recv_sem=c_rsem.at[j, i],
            device_id=(groups[j], src), device_id_type=MESH).wait_recv()

    for j in (1, 2, 3, 0):
        for i in range(crs_size):
            if j or i:
                c_copy(j, i).start()

    def row(p, extra=0):
        return pl.multiple_of(p * part + extra, 8)

    def f_pieces(i):
        to = lax.rem(c + i, crs_size)
        nx = lax.rem(to + 1, crs_size)
        pv = lax.rem(to + crs_size - 1, crs_size)
        return to, (
            (row(to), 0, part, g),
            (row(nx), up, EDGE, g),
            (row(pv, part - EDGE), down, EDGE, g),
            (row(to), off_x, part, across),
            (row(to), off_p, part, after),
            (row(to), off_n, part, before),
        )

    def f_copy(i, n):
        to, pieces = f_pieces(i)
        start, place, size, where = pieces[n]
        return pltpu.make_async_remote_copy(
            src_ref=factor.at[pl.ds(start, size), :],
            dst_ref=fcat.at[c, pl.ds(place, size), :],
            send_sem=f_ssem.at[i, n], recv_sem=f_rsem.at[i, n],
            device_id=(where, to), device_id_type=MESH)

    def f_wait(i, n):
        to, pieces = f_pieces(i)
        start, place, size, where = pieces[n]
        src = lax.rem(c + crs_size - i, crs_size)
        pltpu.make_async_remote_copy(
            src_ref=factor.at[pl.ds(start, size), :],
            dst_ref=fcat.at[src, pl.ds(place, size), :],
            send_sem=f_ssem.at[i, n], recv_sem=f_rsem.at[i, n],
            device_id=(where, to), device_id_type=MESH).wait_recv()

    for other in outer:
        signal(met, other)

    loads[5].wait()
    span = LANES // part
    blocks = fown.shape[0]
    for b in range(blocks):
        held = factor[b * span * part:min((b + 1) * span, crs_size) * part, :]
        if held.shape[0] < LANES:
            held = jnp.concatenate(
                [held, jnp.zeros((LANES - held.shape[0], held.shape[1]), jnp.float32)], axis=0)
        fown[b] = both(held)

    for j in (0, 1, 2, 3):
        for i in range(crs_size):
            if j or i:
                c_wait(j, i)

    lane = lax.broadcasted_iota(jnp.int32, (nrhs, LANES), 1)

    def rolled(value, by):
        return pltpu.roll(value, (LANES - by) % LANES, 1) if by % LANES else value

    total = jnp.zeros((nrhs, factor.shape[1]), jnp.float32)
    for b in range(blocks):
        group_rhs = jnp.zeros((nrhs, LANES), jnp.float32)
        for p in range(b * span, min((b + 1) * span, crs_size)):
            at = (p - b * span) * part
            low = c_recv[0, (p - 1) % crs_size]
            high = c_recv[0, (p + 1) % crs_size]
            rhs = rolled(c_recv[0, p], -at)
            rhs = rhs + jnp.where(lane < at + EDGE, rolled(low, up - at), 0.0)
            rhs = rhs + jnp.where(
                lane >= at + part - EDGE, rolled(high, down - (at + part - EDGE)), 0.0)
            rhs = rhs + rolled(c_recv[1, p], off_x - at)
            rhs = rhs + rolled(c_recv[2, p], off_n - at)
            rhs = rhs + rolled(c_recv[3, p], off_p - at)
            group_rhs = jnp.where((lane >= at) & (lane < at + part), rhs, group_rhs)
        total = total + twice(group_rhs, fown[b])

    chunk = factor.shape[1] // parts
    for q in range(parts):
        for r in range(nrhs):
            rs_send[q * nrhs + r] = total[r:r + 1, q * chunk:(q + 1) * chunk]

    def rs_copy(i):
        to = lax.rem(g + i, sub_size)
        return pltpu.make_async_remote_copy(
            src_ref=rs_send.at[to], dst_ref=rs_recv.at[g],
            send_sem=rs_ssem.at[i], recv_sem=rs_rsem.at[i],
            device_id=(to, c), device_id_type=MESH)

    def rs_wait(i):
        src = lax.rem(g + sub_size - i, sub_size)
        pltpu.make_async_remote_copy(
            src_ref=rs_send.at[src], dst_ref=rs_recv.at[src],
            send_sem=rs_ssem.at[i], recv_sem=rs_rsem.at[i],
            device_id=(src, c), device_id_type=MESH).wait_recv()

    pl.semaphore_wait(met, len(outer))
    each(sub_size - 1, lambda i: rs_copy(i + 1).start())
    moves = [(i, n) for i in range(crs_size) for n in range(6) if i or n > 2]
    for i, n in moves:
        f_copy(i, n).start()
    _, pieces = f_pieces(0)
    for start, place, size, _ in pieces[:3]:
        fcat[c, pl.ds(place, size), :] = factor[pl.ds(start, size), :]

    rs_recv[g] = rs_send[g]
    each(sub_size - 1, lambda i: rs_wait(i + 1))
    mine = rs_recv[0]
    for q in range(1, sub_size):
        mine = mine + rs_recv[q]
    ag_send[...] = mine

    def ag_copy(i):
        return pltpu.make_async_remote_copy(
            src_ref=ag_send, dst_ref=panel.at[c, g],
            send_sem=ag_ssem.at[i], recv_sem=ag_rsem.at[i],
            device_id=rank(i), device_id_type=MESH)

    def ag_wait(i):
        fg, fcr = rank(devices - i)
        pltpu.make_async_remote_copy(
            src_ref=ag_send, dst_ref=panel.at[fcr, fg],
            send_sem=ag_ssem.at[i], recv_sem=ag_rsem.at[i],
            device_id=(fg, fcr), device_id_type=MESH).wait_recv()

    each(devices - 1, lambda i: ag_copy(i + 1).start())
    panel[c, g] = mine
    for i, n in moves:
        f_wait(i, n)
    for p in range(crs_size):
        fpair[p] = both(fcat[p])
    each(devices - 1, lambda i: ag_wait(i + 1))

    amps = jnp.zeros((2 * nrhs, 2 * LANES), jnp.float32)
    for p in range(crs_size):
        for q in range(parts):
            rows = panel[p, q * nrhs:(q + 1) * nrhs].reshape(nrhs, chunk)
            amps = amps + dot(both(rows), fpair[p, :, q * chunk:(q + 1) * chunk], NT)
    amps = quarters(amps)
    for s in range(subs):
        out_h[:, s, :] = twice(amps, pair[:, s * width:(s + 1) * width])

    for j in range(4):
        for i in range(crs_size):
            if j or i:
                c_copy(j, i).wait_send()
    for i, n in moves:
        f_copy(i, n).wait_send()
    each(sub_size - 1, lambda i: rs_copy(i + 1).wait_send())
    each(devices - 1, lambda i: ag_copy(i + 1).wait_send())


def body(sub_size, crs_size, mult, own, nbr, face, nlist, factor):
    nk, subs, width = own.shape
    nrhs = mult.shape[0]
    part = nk * subs
    blocks = -(-crs_size // (LANES // part))
    cols = factor.shape[1]
    chunk = cols * nrhs // sub_size
    f32 = jnp.float32
    dma = pltpu.SemaphoreType.DMA
    bf16 = jnp.bfloat16
    hbm = pl.BlockSpec(memory_space=pl.ANY)
    names = nlist.T
    applied = pl.pallas_call(
        functools.partial(kernel, sub_size, crs_size),
        out_shape=pltpu.VMEM(mult.shape, mult.dtype),
        in_specs=[hbm] * 6,
        out_specs=pl.BlockSpec(memory_space=pltpu.VMEM),
        scratch_shapes=[
            pltpu.VMEM(mult.shape, f32), pltpu.VMEM(own.shape, f32), pltpu.VMEM(nbr.shape, f32),
            pltpu.VMEM(face.shape, face.dtype), pltpu.SMEM(names.shape, names.dtype),
            pltpu.VMEM(factor.shape, f32),
            pltpu.VMEM((LANES, subs * width), f32),
            pltpu.VMEM((2 * LANES, subs * width), bf16),
            pltpu.VMEM((nrhs, LANES), f32),
            pltpu.VMEM((4, crs_size, nrhs, LANES), f32),
            pltpu.VMEM((crs_size, LANES, cols), f32),
            pltpu.VMEM((blocks, 2 * LANES, cols), bf16),
            pltpu.VMEM((crs_size, 2 * LANES, cols), bf16),
            pltpu.VMEM((sub_size, 1, chunk), f32),
            pltpu.VMEM((sub_size, 1, chunk), f32),
            pltpu.VMEM((1, chunk), f32),
            pltpu.VMEM((crs_size, sub_size, 1, chunk), f32),
            dma((4, crs_size)), dma((4, crs_size)),
            dma((crs_size, 6)), dma((crs_size, 6)),
            dma((sub_size,)), dma((sub_size,)),
            dma((sub_size * crs_size,)), dma((sub_size * crs_size,)), dma((6,)),
            pltpu.SemaphoreType.REGULAR,
        ],
        compiler_params=pltpu.CompilerParams(collective_id=0, has_side_effects=True),
    )(mult, own, nbr, face, names, factor)
    return mult - applied


def solution(mesh):
    placed = (
        P(None, ("sub", "crs"), None),
        P(None, ("sub", "crs"), None),
        P(None, ("sub", "crs"), None),
        P(("sub", "crs"), None),
        P(),
        P("sub", "crs"),
    )
    return jax.shard_map(
        functools.partial(body, mesh.shape["sub"], mesh.shape["crs"]),
        mesh=mesh, in_specs=placed, out_specs=P(None, ("sub", "crs"), None), check_vma=False
    )
```
